256 devices in a mesh: fsdp: 64 (over y, z, core), refresh: 4 (over x).
Axes of the slice: x: 4, y: 4, z: 8, core: 2. Of those that a mesh axis runs over, the one named last changes fastest.
Arguments:
- gradient: bfloat16 [4, 192, 65536], P('refresh', None, 'fsdp'), may hold values from -6 to 6
- owner: int32 [4, 192, 1], P('refresh'), may hold values from 0 to 63; in each aligned block of 192 rows (0 to 191, 192 to 383, ..., all dimensions but the last counted through in order) at most 4 rows name the same one
- rotation: int32 [64], replicated, may hold values from 0 to 3
- left_factor: float32 [4, 256, 256, 256], P('refresh', 'fsdp'), may hold values from -1 to 8, as said below
- right_factor: float32 [4, 256, 256, 256], P('refresh', 'fsdp'), may hold values from -1 to 8, as said below
- left_basis: float32 [4, 256, 256, 256], P('refresh', 'fsdp'), may hold values from -1 to 1, as said below
- right_basis: float32 [4, 256, 256, 256], P('refresh', 'fsdp'), may hold values from -1 to 1, as said below
- moment: float32 [4, 256, 256, 256], P('refresh', 'fsdp'), may hold values from -4 to 4
- second_moment: float32 [4, 256, 256, 256], P('refresh', 'fsdp'), may hold values from 0.05 to 2
Outputs:
- direction: float32 [4, 192, 65536], P('refresh', None, 'fsdp')
- left_factor_new: float32 [4, 256, 256, 256], P('refresh', 'fsdp')
- right_factor_new: float32 [4, 256, 256, 256], P('refresh', 'fsdp')
- left_basis_new: float32 [4, 256, 256, 256], P('refresh', 'fsdp')
- right_basis_new: float32 [4, 256, 256, 256], P('refresh', 'fsdp')
- moment_new: float32 [4, 256, 256, 256], P('refresh', 'fsdp')
- second_moment_new: float32 [4, 256, 256, 256], P('refresh', 'fsdp')
The draws below stay inside these ranges and needn't reach their ends.
Inputs may be any that keep to these rules, and one draw needn't show every extreme that they name: Within each group no owner is named by more than 4 blocks, a bound that some block reaches; some owner is named by at least one block. The state of block b lies in slot s(b) of the steps; the states of slots that no block takes are carried unchanged. `left_factor`: each slot's factor is symmetric positive definite. `right_factor`: each slot's factor is symmetric positive definite. `left_basis`: each slot's basis is orthogonal. `right_basis`: each slot's basis is orthogonal.
All inputs are finite; a program needn't handle non-finite values.
Results may differ from the reference program's by a relative error of at most 0.0003.
Values may be sent and summed in bfloat16 or wider, within the bound.
No kernel may reach another device: no remote copies, remote signals or barrier semaphores. Data moves between devices by JAX's collectives and lax.ppermute only.
A program may use at most 64 MiB of HBM per device.

```python
import math
import jax
import jax.numpy as jnp
import numpy as np
from jax import lax

BS = 256
CAP = 4
GROUPS = 4
BLOCKS = 192
SLOTS = 256
N_FSDP = 64
N_REFRESH = 4


def factor_matrix(key, lowest, highest, spread):
    first, second = jax.random.split(key)
    shape = (GROUPS, SLOTS, BS, BS)
    noise = jax.random.normal(first, shape, jnp.float32) * (spread / math.sqrt(2.0 * BS))
    symmetric = noise + jnp.swapaxes(noise, 2, 3)
    diagonal = jnp.exp(jax.random.uniform(second, shape[:3], jnp.float32, math.log(lowest), math.log(highest)))
    return symmetric + diagonal[..., None] * jnp.eye(BS, dtype=jnp.float32)


def basis_matrix(key):
    noise = jax.random.normal(key, (GROUPS, SLOTS, BS, BS), jnp.float32)
    orthogonal, _ = jnp.linalg.qr(noise)
    return orthogonal


def draw_left_factor(key, part):
    return factor_matrix(jax.random.fold_in(key, 11), 1.0, 4.0, 0.4)


def draw_right_factor(key, part):
    return factor_matrix(jax.random.fold_in(key, 23), 1.0, 4.0, 0.4)


def draw_left_basis(key, part):
    return basis_matrix(jax.random.fold_in(key, 37))


def draw_right_basis(key, part):
    return basis_matrix(jax.random.fold_in(key, 41))


def set_ends(drawn, key, smallest, high):
    longest = drawn.shape.index(max(drawn.shape))
    spots = []
    for shift in (0, 1):
        where = [jax.random.randint(jax.random.fold_in(key, axis), (), 0, length) for axis, length in enumerate(drawn.shape)]
        where[longest] = (where[longest] + shift) % drawn.shape[longest]
        spots.append(tuple(where))
    return drawn.at[spots[0]].set(smallest).at[spots[1]].set(high)


def level_of(own_key, dims, shards, low, largest):
    def one(axis_at, parts):
        draws = jax.random.uniform(jax.random.fold_in(jax.random.fold_in(own_key, 6), axis_at), (parts,), jnp.float32, low / len(shards), largest / len(shards))
        return jnp.repeat(jnp.exp(draws), dims[axis_at] // parts).reshape((-1,) + (1,) * (len(dims) - axis_at - 1))

    loudness = one(*shards[0])
    for cut in shards[1:]:
        loudness = loudness * one(*cut)
    return loudness


def shared_out(own_key, own, number, rows, count, top, most, skew):
    sequence = jax.random.permutation(own_key, count)
    packed, common = portions_of(count, rows * top, most, skew, True), portions_of(count, rows * top, most, skew, False)
    places = jnp.arange(count)

    def named(sizes, turn):
        used = int((sizes > 0).sum())
        fixed = max(1, used // 4)
        moved = fixed + (places - fixed + turn * (used - fixed)) % max(1, count - fixed)
        return jnp.zeros((count,), jnp.int32).at[sequence[jnp.where(places < fixed, places, moved)]].set(jnp.asarray(sizes, jnp.int32))

    sizes = jnp.where(number % 4 == 0, named(packed, number // 4), named(common, number - number // 4 - 1))
    mixed = jax.random.permutation(jax.random.fold_in(own, 3), count)
    donor, taker = mixed[0:count // 2 * 2:2], mixed[1:count // 2 * 2:2]
    margin = jnp.minimum(sizes[donor] - 1, most - sizes[taker]) // 2
    margin = jnp.where((donor == sequence[0]) | (taker == sequence[0]) | (sizes[taker] == 0), 0, jnp.maximum(margin, 0))
    moved = jax.random.randint(jax.random.fold_in(own, 4), (count // 2,), 0, 1 << 20) % (margin + 1)
    sizes = sizes.at[donor].add(-moved).at[taker].add(moved)
    items = jnp.searchsorted(jnp.cumsum(sizes), jnp.arange(rows * top), side="right").astype(jnp.int32)
    table = items.reshape(top, rows).T
    table = table[jax.random.permutation(jax.random.fold_in(own, 1), rows)]
    turn = jax.random.randint(jax.random.fold_in(own, 2), (rows, 1), 0, top)
    return jnp.take_along_axis(table, (jnp.arange(top)[None, :] + turn) % top, axis=1)


def portions_of(amount, total, bound, slope, full):
    loads = [(1 << 20) // math.isqrt(rank ** slope) + 1 for rank in range(1, amount + 1)]
    largest = bound if full else min(bound, max(-(-total // amount), total * loads[0] // sum(loads)))
    least = 1 if total - largest >= amount - 1 else 0
    holding, surplus = [largest] + [least] * (amount - 1), total - largest - least * (amount - 1)
    while surplus > 0:
        free = [i for i in range(1, amount) if holding[i] < largest] or [i for i in range(1, amount) if holding[i] < bound]
        mass, left = sum([loads[i] for i in free]), surplus
        for i in free:
            more = min(bound - holding[i], max(1, left * loads[i] // mass), surplus)
            holding[i] = holding[i] + more
            surplus = surplus - more
    return np.array(holding)


def centred(rng, shape, width, bound, pieces=(), kind=jnp.bfloat16):
    drawn = width * jax.random.normal(rng, shape, jnp.float32)
    if pieces:
        drawn = drawn * level_of(rng, shape, pieces, -0.22, 0.18)
    return jnp.clip(drawn, -bound, bound).astype(kind)


def setup_inputs(seed: int = 0) -> dict:
    streams_of = jax.random.split(jax.random.key(seed), 10)
    gradient = centred(streams_of[0], (GROUPS, BLOCKS, BS * BS), 1.0, 6.0, ((0, 4), (2, 64)))
    owner_keys = jax.random.split(jax.random.fold_in(streams_of[1], 1), GROUPS * BLOCKS // BLOCKS)
    owner_turns = jax.random.permutation(jax.random.fold_in(streams_of[1], 3), GROUPS * BLOCKS // BLOCKS)
    owner = jax.vmap(lambda own, number: shared_out(jax.random.fold_in(streams_of[1], 2), own, number, BLOCKS, N_FSDP, 1, CAP, 1))(owner_keys, owner_turns).reshape((GROUPS, BLOCKS, 1))
    rotation = set_ends(jax.random.randint(streams_of[2], (N_FSDP,), 0, N_REFRESH), jax.random.fold_in(streams_of[2], 1), 0, N_REFRESH - 1).astype(jnp.int32)
    left_factor = draw_left_factor(jax.random.fold_in(streams_of[9], 71), 0)
    right_factor = draw_right_factor(jax.random.fold_in(streams_of[9], 71), 0)
    left_basis = draw_left_basis(jax.random.fold_in(streams_of[9], 71), 0)
    right_basis = draw_right_basis(jax.random.fold_in(streams_of[9], 71), 0)
    moment = centred(streams_of[7], (GROUPS, SLOTS, BS, BS), 0.5, 4.0, ((0, 4), (1, 64)), jnp.float32)
    second_moment = jnp.clip(jnp.exp(math.log(2.0) - 3.6888794 * jax.random.uniform(streams_of[8], (GROUPS, SLOTS, BS, BS), jnp.float32) ** level_of(streams_of[8], (GROUPS, SLOTS, BS, BS), ((0, 4), (1, 64)), -0.2, 0.2)), 0.05, 2.0)
    return dict(gradient=gradient, owner=owner, rotation=rotation, left_factor=left_factor, right_factor=right_factor, left_basis=left_basis, right_basis=right_basis, moment=moment, second_moment=second_moment)


HIGHEST = lax.Precision.HIGHEST
EPSILON = 1e-08

def slot_rows(owners):
    onehot = (owners[:, None] == jnp.arange(N_FSDP, dtype=jnp.int32)[None, :]).astype(jnp.int32)
    before = jnp.cumsum(onehot, axis=0) - onehot
    return (owners * CAP + lax.optimization_barrier(jnp.sum(before * onehot, axis=1))).astype(jnp.int32)

def power_step(factor, basis):
    image = jnp.einsum('sij,sjk->sik', factor, basis, precision=HIGHEST)
    gram = jnp.einsum('sji,sjk->sik', image, image, precision=HIGHEST)
    lower = jnp.linalg.cholesky(gram)
    solved = jax.scipy.linalg.solve_triangular(lower, jnp.swapaxes(image, 1, 2), lower=True)
    return jnp.swapaxes(solved, 1, 2)

def reference(gradient, owner, rotation, left_factor, right_factor, left_basis, right_basis, moment, second_moment):
    target = jax.vmap(slot_rows)(owner[:, :, 0])
    rows = jnp.arange(GROUPS, dtype=jnp.int32)[:, None]
    slotted = jnp.zeros((GROUPS, SLOTS, BS * BS), jnp.bfloat16).at[rows, target].set(gradient)
    live = jnp.zeros((GROUPS, SLOTS), jnp.bool_).at[rows, target].set(True)
    keep = live[:, :, None, None]
    wide = slotted.reshape(GROUPS, SLOTS, BS, BS).astype(jnp.float32)
    gram_left = jnp.einsum('gsij,gskj->gsik', wide, wide, precision=HIGHEST)
    gram_right = jnp.einsum('gsji,gsjk->gsik', wide, wide, precision=HIGHEST)
    left_new = 0.95 * left_factor + 0.05 / BS * gram_left
    right_new = 0.95 * right_factor + 0.05 / BS * gram_right
    moment_next = 0.9 * moment + 0.1 * wide

    def rotate(middle):
        inner = jnp.einsum('gsji,gsjk->gsik', left_basis, middle, precision=HIGHEST)
        return jnp.einsum('gsij,gsjk->gsik', inner, right_basis, precision=HIGHEST)
    turned = rotate(wide)
    turned_moment = rotate(moment_next)
    second_next = 0.95 * second_moment + 0.05 * turned * turned
    scaled = turned_moment / (jnp.sqrt(second_next) + EPSILON)
    backed = jnp.einsum('gsij,gsjk->gsik', left_basis, scaled, precision=HIGHEST)
    update = jnp.einsum('gsij,gskj->gsik', backed, right_basis, precision=HIGHEST)
    direction = update.reshape(GROUPS, SLOTS, BS * BS)[rows, target]
    owner_index = jnp.arange(N_FSDP, dtype=jnp.int32)
    first_slot = (owner_index * CAP).astype(jnp.int32)
    chosen = rotation.astype(jnp.int32)
    fresh_left = power_step(left_new[chosen, first_slot], left_basis[chosen, first_slot])
    fresh_right = power_step(right_new[chosen, first_slot], right_basis[chosen, first_slot])
    fresh_left = jnp.repeat(fresh_left, CAP, axis=0)
    fresh_right = jnp.repeat(fresh_right, CAP, axis=0)
    slot_index = jnp.arange(SLOTS, dtype=jnp.int32)
    slot_chosen = chosen[slot_index // CAP]
    leading = slot_index % CAP == 0
    picked = ((jnp.arange(GROUPS, dtype=jnp.int32)[:, None] == slot_chosen[None, :]) & leading[None, :])[:, :, None, None] & keep
    left_basis_new = jnp.where(picked, fresh_left[None], left_basis)
    right_basis_new = jnp.where(picked, fresh_right[None], right_basis)
    return (direction, jnp.where(keep, left_new, left_factor), jnp.where(keep, right_new, right_factor), left_basis_new, right_basis_new, jnp.where(keep, moment_next, moment), jnp.where(keep, second_next, second_moment))
```

```python
import functools

import jax
import jax.numpy as jnp
from jax import lax
from jax.experimental import pallas as pl
from jax.experimental.pallas import tpu as pltpu
from jax.sharding import PartitionSpec as P

HIGHEST = lax.Precision.HIGHEST
EPSILON = 1e-08
F32 = jnp.float32
BF16 = jnp.bfloat16
PANEL = 32
SUB = 8

NN = (((1,), (0,)), ((), ()))
NT = (((1,), (1,)), ((), ()))
TN = (((0,), (0,)), ((), ()))


def mul(a, b, dims=NN):
    return lax.dot_general(a, b, dims, preferred_element_type=F32)


def split2(x):
    high = x.astype(BF16)
    return high, (x - high.astype(F32)).astype(BF16)


def split3(x):
    high = x.astype(BF16)
    rest = x - high.astype(F32)
    middle = rest.astype(BF16)
    return high, middle, (rest - middle.astype(F32)).astype(BF16)


def mul3(a, b, dims=NN):
    return mul(a[0], b[0], dims) + (mul(a[0], b[1], dims) + mul(a[1], b[0], dims))


def params(mib):
    return pltpu.CompilerParams(vmem_limit_bytes=mib * 1024 * 1024)


def cost(flops, size):
    return pl.CostEstimate(flops=flops, bytes_accessed=size, transcendentals=0)


def in_hbm(x):
    return pltpu.with_memory_space_constraint(x, pltpu.HBM)


def ranks(row):
    blocks = row.shape[1]
    down = lax.broadcasted_iota(jnp.int32, (blocks, blocks), 0)
    across = lax.broadcasted_iota(jnp.int32, (blocks, blocks), 1)
    column = jnp.sum(jnp.where(down == across, row, 0.0), axis=1, keepdims=True)
    return column, row, down, across


def place_kernel(cap, owner_ref, gradient_ref, out_ref, scratch):
    slots = scratch.shape[0] // 8
    column, row, before, after = ranks(owner_ref[...].astype(F32))
    earlier = jnp.where((column == row) & (before < after), 1.0, 0.0)
    target = row * cap + jnp.sum(earlier, axis=0, keepdims=True)
    number = lax.broadcasted_iota(jnp.int32, (slots, target.shape[1]), 0).astype(F32)
    placing = jnp.where(number == target, 1.0, 0.0).astype(BF16)
    for part in range(8):
        lanes = slice(128 * part, 128 * part + 128)
        scratch[pl.ds(part, slots, stride=8), :] = mul(placing, gradient_ref[:, lanes])
    out_ref[...] = scratch[...].astype(BF16)


def ahead_kernel(
    cap, owner_ref, left_ref, right_ref, moment_ref,
    lh_ref, ll_ref, th_ref, tl_ref, rh_ref, rl_ref, turned_ref, pick_ref,
):
    left = left_ref[0]
    lh_ref[0], ll_ref[0] = split2(left)
    flipped = split2(left.T)
    th_ref[0], tl_ref[0] = flipped
    right = split2(right_ref[0])
    rh_ref[0], rl_ref[0] = right
    inner = mul3(flipped, split2(moment_ref[0]))
    turned_ref[0] = mul3(split2(inner), right)

    @pl.when(pl.program_id(0) == 0)
    def _():
        column, row, before, after = ranks(owner_ref[...].astype(F32))
        earlier = jnp.where((column == row) & (after < before), 1.0, 0.0)
        target = column * cap + jnp.sum(earlier, axis=1, keepdims=True)
        blocks, slots = pick_ref.shape
        number = lax.broadcasted_iota(jnp.int32, (blocks, slots), 1).astype(F32)
        pick_ref[...] = jnp.where(number == target, 1.0, 0.0).astype(BF16)


def update_kernel(
    x_ref, lh_hbm, ll_hbm, th_hbm, tl_hbm, rh_hbm, rl_hbm, ahead_hbm, second_hbm, count_ref,
    block_ref, next_ref, out_ref,
    lh_ref, ll_ref, th_ref, tl_ref, rh_ref, rl_ref, ahead_ref, second_ref, scratch, arrivals,
):
    width = block_ref.shape[1]
    half = 2 * width
    pair = range(2)
    step = pl.program_id(0)
    kept = (th_hbm, tl_hbm, rh_hbm, rl_hbm, ahead_hbm, second_hbm, lh_hbm, ll_hbm)
    here = (th_ref, tl_ref, rh_ref, rl_ref, ahead_ref, second_ref, lh_ref, ll_ref)

    def copies(at):
        return [
            pltpu.make_async_copy(
                source.at[pl.ds(2 * at, 2)], target.at[pl.ds(2 * at, 2)], arrivals.at[n, at]
            )
            for n, (source, target) in enumerate(zip(kept, here))
        ]

    @pl.when(step == 0)
    def _():
        for at in range(2):
            for copy in copies(at):
                copy.start()

    wide = x_ref[...].astype(F32)
    for s in pair:
        scratch[s * half : (s + 1) * half, :] = wide[:, 8 * s : 8 * s + 8, :].reshape(half, 128)
    blocks = []
    for s in pair:
        columns = [scratch[pl.ds(s * half + h, width, stride=2), :] for h in range(2)]
        blocks.append(jnp.concatenate(columns, axis=1).astype(BF16))
        block_ref[s] = blocks[s]
    for copy in copies(step):
        copy.wait()
    slot = [2 * step + s for s in pair]
    right = [(rh_ref[slot[s]], rl_ref[slot[s]]) for s in pair]
    inner = [mul(th_ref[slot[s]], blocks[s]) + mul(tl_ref[slot[s]], blocks[s]) for s in pair]
    turned = [mul3(split2(inner[s]), right[s]) for s in pair]
    scaled = []
    for s in pair:
        second = second_ref[slot[s]]
        fresh = 0.95 * second + 0.05 * turned[s] * turned[s]
        next_ref[s] = jnp.where(slot[s] < count_ref[0], fresh, second)
        moment = 0.9 * ahead_ref[slot[s]] + 0.1 * turned[s]
        scaled.append(moment / (jnp.sqrt(fresh) + EPSILON))
    backed = [mul3((lh_ref[slot[s]], ll_ref[slot[s]]), split2(scaled[s])) for s in pair]
    update = [mul3(split2(backed[s]), right[s], NT) for s in pair]
    for s in pair:
        for h in range(2):
            scratch[pl.ds(s * half + h, width, stride=2), :] = update[s][:, 128 * h : 128 * h + 128]
    for s in pair:
        part = scratch[s * half : (s + 1) * half, :]
        out_ref[:, 8 * s : 8 * s + 8, :] = part.reshape(out_ref.shape[0], 8, 128)


def state_kernel(
    block_ref, left_ref, right_ref, moment_ref, count_ref, left_out, right_out, moment_out
):
    width = block_ref.shape[1]
    block = block_ref[0]
    live = pl.program_id(0) < count_ref[0]
    left, right, moment = left_ref[0], right_ref[0], moment_ref[0]
    left_new = 0.95 * left + 0.05 / width * mul(block, block, NT)
    right_new = 0.95 * right + 0.05 / width * mul(block, block, TN)
    left_out[0] = jnp.where(live, left_new, left)
    right_out[0] = jnp.where(live, right_new, right)
    moment_out[0] = jnp.where(live, 0.9 * moment + 0.1 * block.astype(F32), moment)


def panel_step(work, first):
    width = work.shape[0]
    lead = first // 128 * 128
    groups = PANEL // SUB
    rows = [work[first + SUB * i : first + SUB * i + SUB, lead:] for i in range(groups)]
    lanes = rows[0].shape[1]
    below = lax.broadcasted_iota(jnp.int32, (SUB, 128), 0)
    done = []
    for i in range(groups):
        at = first - lead + SUB * i
        columns = [
            [jnp.broadcast_to(rows[g][:, at + j : at + j + 1], (SUB, 128)) for g in range(i, groups)]
            for j in range(SUB)
        ]
        mine = rows[i]
        scale = jnp.zeros((SUB, 128), F32)
        factors = []
        for j in range(SUB):
            root = lax.rsqrt(jnp.broadcast_to(columns[j][0][j : j + 1, :], (SUB, 128)))
            factor = [c * root for c in columns[j]]
            factors.append(factor)
            scale = jnp.where(below == j, root, scale)
            for m in range(j + 1, SUB):
                there = jnp.broadcast_to(factor[0][m : m + 1, :], (SUB, 128))
                columns[m] = [c - f * there for c, f in zip(columns[m], factor)]
            if j + 1 < SUB:
                lower = jnp.where(below > j, factor[0] * root, 0.0)
                pivot = jnp.broadcast_to(mine[j : j + 1, :], (SUB, lanes))
                mine = mine - jnp.concatenate([lower] * (lanes // 128), axis=1) * pivot
        mine = mine * jnp.concatenate([scale] * (lanes // 128), axis=1)
        done.append(mine)
        for j in range(SUB):
            pivot = jnp.broadcast_to(mine[j : j + 1, :], (SUB, lanes))
            for g in range(i + 1, groups):
                factor = jnp.concatenate([factors[j][g - i]] * (lanes // 128), axis=1)
                rows[g] = rows[g] - factor * pivot
    solved = jnp.concatenate(done, axis=0)
    work[first : first + PANEL, width:] = solved[:, width - lead :]
    later = first + PANEL
    if later < width:
        start = later // 128 * 128
        kept = solved[:, start - lead :]
        high, middle, low = split3(kept)
        reach = width - start
        sides = [part[:, :reach] for part in (high, high, middle, high, low, middle)]
        product = mul(
            jnp.concatenate(sides, axis=0),
            jnp.concatenate([high, middle, high, low, high, middle], axis=0),
            TN,
        )
        work[later:, start:] = work[later:, start:] - product[later - start :, :]


def basis_kernel(
    left_ref, right_ref, left_basis_ref, right_basis_ref, flag_ref, left_out, right_out, one, two
):
    width = left_ref.shape[1]
    works = (one, two)
    factors = (left_ref, right_ref)
    bases = (left_basis_ref, right_basis_ref)
    outs = (left_out, right_out)

    @pl.when(pl.program_id(0) == 0)
    def _():
        for work, factor, basis in zip(works, factors, bases):
            image = lax.dot_general(factor[0], basis[0], NN, precision=HIGHEST, preferred_element_type=F32)
            flipped = image.T
            work[:, width:] = flipped
            work[:, :width] = lax.dot_general(flipped, image, NN, precision=HIGHEST, preferred_element_type=F32)
        for first in range(0, width, PANEL):
            for work in works:
                panel_step(work, first)
        for work, basis, out in zip(works, bases, outs):
            out[0] = jnp.where(flag_ref[0] > 0, work[:, width:].T, basis[0])

    @pl.when(pl.program_id(0) > 0)
    def _():
        for basis, out in zip(bases, outs):
            out[0] = basis[0]


def pick_kernel(returned_ref, pick_ref, out_ref):
    slots = pick_ref.shape[1]
    pick = pick_ref[...]
    for part in range(8):
        high, middle, low = split3(returned_ref[pl.ds(part, slots, stride=8), :])
        out_ref[:, 128 * part : 128 * part + 128] = mul(pick, high) + (mul(pick, middle) + mul(pick, low))


def body(
    gradient,
    owner,
    rotation,
    left_factor,
    right_factor,
    left_basis,
    right_basis,
    moment,
    second_moment,
):
    shards = lax.axis_size("fsdp")
    mine = lax.axis_index("fsdp")
    group = lax.axis_index("refresh")
    cap, width = left_factor.shape[1:3]
    slots = shards * cap
    blocks = gradient.shape[1]
    owners = owner.reshape(1, blocks)
    square = (cap, width, width)
    one_slot = pl.BlockSpec((1, width, width), lambda s: (s, 0, 0))
    two_slots = pl.BlockSpec((2, width, width), lambda s: (s, 0, 0))
    smem = pl.BlockSpec(memory_space=pltpu.SMEM)
    chunk = cap * 8
    cube = 2 * width**3


    outgoing = pl.pallas_call(
        functools.partial(place_kernel, cap),
        out_shape=jax.ShapeDtypeStruct((slots * 8, 128), BF16),
        scratch_shapes=[pltpu.VMEM((slots * 8, 128), F32)],
        compiler_params=params(56),
        cost_estimate=cost(2 * slots * blocks * 1024, 1 << 20),
        name="place",
    )(owners, gradient[0])
    arrived = lax.all_to_all(
        outgoing.reshape(shards, chunk, 128), "fsdp", split_axis=0, concat_axis=0, tiled=True
    )

    lh, ll, th, tl, rh, rl, ahead, pick = pl.pallas_call(
        functools.partial(ahead_kernel, cap),
        grid=(cap,),
        in_specs=[pl.BlockSpec((1, blocks), lambda s: (0, 0))] + [one_slot] * 3,
        out_specs=[one_slot] * 7 + [pl.BlockSpec((blocks, slots), lambda s: (0, 0))],
        out_shape=[jax.ShapeDtypeStruct(square, BF16)] * 6
        + [jax.ShapeDtypeStruct(square, F32), jax.ShapeDtypeStruct((blocks, slots), BF16)],
        compiler_params=params(56),
        cost_estimate=cost(cap * 6 * cube, 7 << 20),
        name="ahead",
    )(owners, left_basis[0], right_basis[0], moment[0])

    count = jnp.sum((owners == mine).astype(jnp.int32)).reshape(1)
    chosen = lax.dynamic_index_in_dim(rotation, mine, 0, keepdims=True)
    flag = ((group == chosen) & (count > 0)).astype(jnp.int32)

    pair_chunk = pl.BlockSpec((shards, chunk // 2, 128), lambda t: (0, t, 0))
    placed, second_new, update = pl.pallas_call(
        update_kernel,
        grid=(cap // 2,),
        in_specs=[pair_chunk] + [pl.BlockSpec(memory_space=pltpu.HBM)] * 8 + [smem],
        out_specs=[two_slots, two_slots, pair_chunk],
        out_shape=[
            jax.ShapeDtypeStruct(square, BF16),
            jax.ShapeDtypeStruct(square, F32),
            jax.ShapeDtypeStruct((shards, chunk, 128), F32),
        ],
        scratch_shapes=[pltpu.VMEM(square, BF16)] * 6
        + [pltpu.VMEM(square, F32)] * 2
        + [pltpu.VMEM((4 * width, 128), F32), pltpu.SemaphoreType.DMA((8, 2))],
        compiler_params=params(32),
        cost_estimate=cost(cap * 11 * cube, 8 << 20),
        name="update",
    )(arrived, *map(in_hbm, (lh, ll, th, tl, rh, rl, ahead, second_moment[0])), count)
    placed = in_hbm(placed)
    returned = lax.all_to_all(update, "fsdp", split_axis=0, concat_axis=0, tiled=True)

    left_new, right_new, moment_new = pl.pallas_call(
        state_kernel,
        grid=(cap,),
        in_specs=[one_slot] * 4 + [smem],
        out_specs=[one_slot] * 3,
        out_shape=[jax.ShapeDtypeStruct(square, F32)] * 3,
        compiler_params=params(56),
        cost_estimate=cost(cap * 8 * cube, 6 << 20),
        name="state",
    )(placed, left_factor[0], right_factor[0], moment[0], count)

    left_basis_new, right_basis_new = pl.pallas_call(
        basis_kernel,
        grid=(cap,),
        in_specs=[pl.BlockSpec((1, width, width), lambda s: (0, 0, 0))] * 2 + [one_slot] * 2 + [smem],
        out_specs=[one_slot] * 2,
        out_shape=[jax.ShapeDtypeStruct(square, F32)] * 2,
        scratch_shapes=[pltpu.VMEM((width, 2 * width), F32)] * 2,
        compiler_params=params(56),
        cost_estimate=cost(400 * cube, 4 << 20),
        name="basis",
    )(left_new, right_new, left_basis[0], right_basis[0], flag)

    direction = pl.pallas_call(
        pick_kernel,
        out_shape=jax.ShapeDtypeStruct((blocks, 1024), F32),
        compiler_params=params(24),
        cost_estimate=cost(6 * slots * blocks * 1024, 2 << 20),
        name="pick",
    )(returned.reshape(slots * 8, 128), pick)
    outs = (direction, left_new, right_new, left_basis_new, right_basis_new, moment_new, second_new)
    return tuple(out[None] for out in outs)


def solution(mesh):
    spread = P("refresh", None, "fsdp")
    state = P("refresh", "fsdp", None, None)
    in_specs = (spread, P("refresh", None, None), P()) + (state,) * 6
    out_specs = (spread,) + (state,) * 6
    return jax.shard_map(body, mesh=mesh, in_specs=in_specs, out_specs=out_specs, check_vma=False)
```
